8 devices in a mesh: fsdp: 8 (over z, y, x, core).
Axes of the slice: x: 2, y: 2, z: 1, core: 2. Of those that a mesh axis runs over, the one named last changes fastest.
Arguments:
- x_in: bfloat16 [8, 768, 1024], P('fsdp')
- positions: int32 [768], replicated
- grad_out: bfloat16 [8, 768, 1024], P('fsdp')
- ln_gamma_1: float32 [1024], P('fsdp')
- w_q_1: bfloat16 [1024, 2048], P('fsdp')
- w_k_1: bfloat16 [1024, 1024], P('fsdp')
- w_v_1: bfloat16 [1024, 1024], P('fsdp')
- w_o_1: bfloat16 [2048, 1024], P('fsdp')
- w_gate_1: bfloat16 [1024, 3072], P('fsdp')
- w_up_1: bfloat16 [1024, 3072], P('fsdp')
- w_down_1: bfloat16 [3072, 1024], P('fsdp')
- q_norm_1: float32 [2048], P('fsdp')
- k_norm_1: float32 [1024], P('fsdp')
- ln_gamma_2: float32 [1024], P('fsdp')
- w_q_2: bfloat16 [1024, 2048], P('fsdp')
- w_k_2: bfloat16 [1024, 1024], P('fsdp')
- w_v_2: bfloat16 [1024, 1024], P('fsdp')
- w_o_2: bfloat16 [2048, 1024], P('fsdp')
- w_gate_2: bfloat16 [1024, 3072], P('fsdp')
- w_up_2: bfloat16 [1024, 3072], P('fsdp')
- w_down_2: bfloat16 [3072, 1024], P('fsdp')
- q_norm_2: float32 [2048], P('fsdp')
- k_norm_2: float32 [1024], P('fsdp')
Outputs:
- output 1: bfloat16 [8, 768, 1024], P('fsdp')
- output 2: bfloat16 [8, 768, 1024], P('fsdp')
- output 3: float32 [1024], P('fsdp')
- output 4: float32 [1024, 2048], P('fsdp')
- output 5: float32 [1024, 1024], P('fsdp')
- output 6: float32 [1024, 1024], P('fsdp')
- output 7: float32 [2048, 1024], P('fsdp')
- output 8: float32 [1024, 3072], P('fsdp')
- output 9: float32 [1024, 3072], P('fsdp')
- output 10: float32 [3072, 1024], P('fsdp')
- output 11: float32 [2048], P('fsdp')
- output 12: float32 [1024], P('fsdp')
- output 13: float32 [1024], P('fsdp')
- output 14: float32 [1024, 2048], P('fsdp')
- output 15: float32 [1024, 1024], P('fsdp')
- output 16: float32 [1024, 1024], P('fsdp')
- output 17: float32 [2048, 1024], P('fsdp')
- output 18: float32 [1024, 3072], P('fsdp')
- output 19: float32 [1024, 3072], P('fsdp')
- output 20: float32 [3072, 1024], P('fsdp')
- output 21: float32 [2048], P('fsdp')
- output 22: float32 [1024], P('fsdp')
All inputs are finite; a program needn't handle non-finite values.
Results may differ from the reference program's by a relative error of at most 0.0186895.
Values are sent between devices in bfloat16 or wider.
A program may use at most 1 GiB of HBM per device.

```python
import functools
import jax
import jax.numpy as jnp
from jax import lax

MODEL_DIM = 1024
NUM_HEADS = 16
KV_HEADS = 8
HEAD_DIM = 128
FFN_DIM = 3072
SEQ_LEN = 768
TOTAL_BATCH = 8

EPSILON = 1e-5
ROPE_THETA = 7.5e7
PARAM_NAMES = ('ln_gamma', 'w_q', 'w_k', 'w_v', 'w_o', 'w_gate', 'w_up', 'w_down', 'q_norm', 'k_norm')


def draw_layer(layer_key):
    sub_keys = jax.random.split(layer_key, 10)
    q_width = NUM_HEADS * HEAD_DIM
    kv_width = KV_HEADS * HEAD_DIM

    def weight(key_w, fan_in, fan_out):
        return (jax.random.normal(key_w, (fan_in, fan_out), jnp.float32) * fan_in ** -0.5).astype(jnp.bfloat16)

    def gain(key_g, width):
        return 1.0 + 0.3 * jax.random.normal(key_g, (width,), jnp.float32)

    return (
        gain(sub_keys[0], MODEL_DIM),
        weight(sub_keys[1], MODEL_DIM, q_width),
        weight(sub_keys[2], MODEL_DIM, kv_width),
        weight(sub_keys[3], MODEL_DIM, kv_width),
        weight(sub_keys[4], q_width, MODEL_DIM),
        weight(sub_keys[5], MODEL_DIM, FFN_DIM),
        weight(sub_keys[6], MODEL_DIM, FFN_DIM),
        weight(sub_keys[7], FFN_DIM, MODEL_DIM),
        gain(sub_keys[8], q_width),
        gain(sub_keys[9], kv_width),
    )


def setup_inputs(seed: int = 0) -> dict:
    root_key = jax.random.key(seed)
    sub_keys = jax.random.split(root_key, 3)
    act_shape = (TOTAL_BATCH, SEQ_LEN, MODEL_DIM)
    pos_gaps = jax.random.randint(sub_keys[1], (SEQ_LEN,), 1, 4, jnp.int32)
    inputs = {
        'x_in': jax.random.normal(sub_keys[0], act_shape, jnp.float32).astype(jnp.bfloat16),
        'positions': (jnp.cumsum(pos_gaps) - pos_gaps[0]).astype(jnp.int32),
        'grad_out': jax.random.normal(sub_keys[2], act_shape, jnp.float32).astype(jnp.bfloat16),
    }
    for layer_index in range(2):
        drawn_params = draw_layer(jax.random.fold_in(root_key, 100 + layer_index))
        for param_name, param_value in zip(PARAM_NAMES, drawn_params):
            inputs[param_name + '_' + str(layer_index + 1)] = param_value
    return inputs


def layer_norm32(values, weight):
    row_mean = jnp.mean(values, axis=-1, keepdims=True)
    centered = values - row_mean
    variance = jnp.mean(centered * centered, axis=-1, keepdims=True)
    return centered * lax.rsqrt(variance + EPSILON) * weight


def rope_tables(positions):
    inv_freq = ROPE_THETA ** (-jnp.arange(0, HEAD_DIM, 2, dtype=jnp.float32) / HEAD_DIM)
    angles = positions.astype(jnp.float32)[:, None] * inv_freq[None, :]
    return jnp.cos(angles), jnp.sin(angles)


def apply_rope(values, cos_tab, sin_tab):
    pair_view = values.reshape(values.shape[:-1] + (HEAD_DIM // 2, 2))
    even_part = pair_view[..., 0]
    odd_part = pair_view[..., 1]
    cos_b = cos_tab[:, None, :]
    sin_b = sin_tab[:, None, :]
    rotated = jnp.stack([even_part * cos_b - odd_part * sin_b, even_part * sin_b + odd_part * cos_b], axis=-1)
    return rotated.reshape(values.shape)


def attention_core(q_raw, k_raw, v_heads, q_norm, k_norm, cos_tab, sin_tab):
    seq_len, n_heads = q_raw.shape[0], q_raw.shape[1]
    n_kv = k_raw.shape[1]
    q_rot = apply_rope(layer_norm32(q_raw, q_norm), cos_tab, sin_tab).astype(jnp.bfloat16)
    k_rot = apply_rope(layer_norm32(k_raw, k_norm), cos_tab, sin_tab).astype(jnp.bfloat16)
    q_grp = q_rot.reshape(seq_len, n_kv, n_heads // n_kv, HEAD_DIM)
    scores = jnp.einsum('qkgd,skd->kgqs', q_grp.astype(jnp.float32), k_rot.astype(jnp.float32)) * HEAD_DIM ** -0.5
    causal = jnp.arange(seq_len)[:, None] >= jnp.arange(seq_len)[None, :]
    attn_prob = jax.nn.softmax(jnp.where(causal, scores, -1e30), axis=-1).astype(jnp.bfloat16)
    context = jnp.einsum('kgqs,skd->qkgd', attn_prob.astype(jnp.float32), v_heads.astype(jnp.float32))
    return context.astype(jnp.bfloat16).reshape(seq_len, n_heads * HEAD_DIM)


def swiglu(gate_proj, up_proj):
    return jax.nn.silu(gate_proj) * up_proj


def layer_forward(stream, params, cos_tab, sin_tab):
    ln_gamma, w_q, w_k, w_v, w_o, w_gate, w_up, w_down, q_norm, k_norm = params
    lead_shape = stream.shape[:-1]
    n_heads = w_q.shape[1] // HEAD_DIM
    n_kv = w_k.shape[1] // HEAD_DIM
    x_f32 = stream.astype(jnp.float32)
    normed = layer_norm32(x_f32, ln_gamma).astype(jnp.bfloat16)
    q_raw = jnp.dot(normed, w_q, preferred_element_type=jnp.float32).reshape(lead_shape + (n_heads, HEAD_DIM))
    k_raw = jnp.dot(normed, w_k, preferred_element_type=jnp.float32).reshape(lead_shape + (n_kv, HEAD_DIM))
    v_heads = jnp.dot(normed, w_v, preferred_element_type=jnp.float32).astype(jnp.bfloat16).reshape(lead_shape + (n_kv, HEAD_DIM))
    attn_out = attention_core(q_raw, k_raw, v_heads, q_norm.reshape(n_heads, HEAD_DIM), k_norm.reshape(n_kv, HEAD_DIM), cos_tab, sin_tab)
    gate_proj = jnp.dot(normed, w_gate, preferred_element_type=jnp.float32)
    up_proj = jnp.dot(normed, w_up, preferred_element_type=jnp.float32)
    hidden = swiglu(gate_proj, up_proj).astype(jnp.bfloat16)
    layer_sum = x_f32 + jnp.dot(attn_out, w_o, preferred_element_type=jnp.float32) + jnp.dot(hidden, w_down, preferred_element_type=jnp.float32)
    saved_acts = (stream, normed, q_raw, k_raw, v_heads, attn_out, gate_proj, up_proj, hidden)
    return layer_sum.astype(jnp.bfloat16), saved_acts


def layer_backward(grad_y, saved_acts, params, cos_tab, sin_tab):
    ln_gamma, w_q, w_k, w_v, w_o, w_gate, w_up, w_down, q_norm, k_norm = params
    stream, normed, q_raw, k_raw, v_heads, attn_out, gate_proj, up_proj, hidden = saved_acts
    seq_len = stream.shape[0]
    n_heads = q_raw.shape[1]
    n_kv = k_raw.shape[1]
    g_w_down = jnp.dot(hidden.T, grad_y, preferred_element_type=jnp.float32)
    g_w_o = jnp.dot(attn_out.T, grad_y, preferred_element_type=jnp.float32)
    d_hidden = jnp.dot(grad_y, w_down.T, preferred_element_type=jnp.float32)
    swiglu_vjp = jax.vjp(swiglu, gate_proj, up_proj)[1]
    d_gate, d_up = swiglu_vjp(d_hidden)
    d_gate = d_gate.astype(jnp.bfloat16)
    d_up = d_up.astype(jnp.bfloat16)
    g_w_gate = jnp.dot(normed.T, d_gate, preferred_element_type=jnp.float32)
    g_w_up = jnp.dot(normed.T, d_up, preferred_element_type=jnp.float32)
    d_attn = jnp.dot(grad_y, w_o.T, preferred_element_type=jnp.float32).astype(jnp.bfloat16)
    core_fn = functools.partial(attention_core, cos_tab=cos_tab, sin_tab=sin_tab)
    core_vjp = jax.vjp(core_fn, q_raw, k_raw, v_heads, q_norm.reshape(n_heads, HEAD_DIM), k_norm.reshape(n_kv, HEAD_DIM))[1]
    d_qraw, d_kraw, d_vheads, g_q_norm, g_k_norm = core_vjp(d_attn)
    d_q = d_qraw.astype(jnp.bfloat16).reshape(seq_len, n_heads * HEAD_DIM)
    d_k = d_kraw.astype(jnp.bfloat16).reshape(seq_len, n_kv * HEAD_DIM)
    d_v = d_vheads.reshape(seq_len, n_kv * HEAD_DIM)
    g_w_q = jnp.dot(normed.T, d_q, preferred_element_type=jnp.float32)
    g_w_k = jnp.dot(normed.T, d_k, preferred_element_type=jnp.float32)
    g_w_v = jnp.dot(normed.T, d_v, preferred_element_type=jnp.float32)
    d_normed = (jnp.dot(d_gate, w_gate.T, preferred_element_type=jnp.float32)
                + jnp.dot(d_up, w_up.T, preferred_element_type=jnp.float32)
                + jnp.dot(d_q, w_q.T, preferred_element_type=jnp.float32)
                + jnp.dot(d_k, w_k.T, preferred_element_type=jnp.float32)
                + jnp.dot(d_v, w_v.T, preferred_element_type=jnp.float32))
    norm_vjp = jax.vjp(layer_norm32, stream.astype(jnp.float32), ln_gamma)[1]
    d_stream, g_ln_gamma = norm_vjp(d_normed)
    grad_x = (grad_y.astype(jnp.float32) + d_stream).astype(jnp.bfloat16)
    grads = (g_ln_gamma, g_w_q, g_w_k, g_w_v, g_w_o, g_w_gate, g_w_up, g_w_down, g_q_norm.reshape(-1), g_k_norm.reshape(-1))
    return grad_x, grads


def reference(x_in, positions, grad_out, ln_gamma_1, w_q_1, w_k_1, w_v_1, w_o_1, w_gate_1, w_up_1, w_down_1, q_norm_1, k_norm_1, ln_gamma_2, w_q_2, w_k_2, w_v_2, w_o_2, w_gate_2, w_up_2, w_down_2, q_norm_2, k_norm_2):
    cos_tab, sin_tab = rope_tables(positions)
    layers = ((ln_gamma_1, w_q_1, w_k_1, w_v_1, w_o_1, w_gate_1, w_up_1, w_down_1, q_norm_1, k_norm_1),
              (ln_gamma_2, w_q_2, w_k_2, w_v_2, w_o_2, w_gate_2, w_up_2, w_down_2, q_norm_2, k_norm_2))
    zero_grads = tuple(tuple(jnp.zeros(param_piece.shape, jnp.float32) for param_piece in layer_params) for layer_params in layers)

    def one_sequence(grad_sums, seq_pair):
        stream, seq_grad = seq_pair
        saved_list = []
        for layer_params in layers:
            stream, saved_acts = layer_forward(stream, layer_params, cos_tab, sin_tab)
            saved_list.append(saved_acts)
        new_sums = list(grad_sums)
        for layer_index in (1, 0):
            seq_grad, grads = layer_backward(seq_grad, saved_list[layer_index], layers[layer_index], cos_tab, sin_tab)
            new_sums[layer_index] = tuple(acc_grad + part_grad for acc_grad, part_grad in zip(grad_sums[layer_index], grads))
        return tuple(new_sums), (stream, seq_grad)

    grad_sums, outputs = lax.scan(one_sequence, zero_grads, (x_in, grad_out))
    return (outputs[0], outputs[1]) + grad_sums[0] + grad_sums[1]
```

```python
import jax
import jax.numpy as jnp
from jax import lax
from jax.experimental import pallas as pl
from jax.experimental.pallas import tpu as pltpu
from jax.sharding import PartitionSpec as P


HEAD_DIM = 128
EPSILON = 1e-5
ROPE_THETA = 7.5e7
AXIS = 'fsdp'
F32 = jnp.float32
BF16 = jnp.bfloat16
VMEM_LIMIT = 60 * 1024 * 1024
CORE_BIT, X_BIT, Y_BIT = 1, 2, 4
ORDER_X_FIRST = (3, 7, 1, 5, 2, 6, 0, 4)
ORDER_Y_FIRST = (5, 7, 1, 3, 4, 6, 0, 2)


def dot_nn(a, b):
    return lax.dot_general(a, b, (((1,), (0,)), ((), ())), preferred_element_type=F32)


def dot_nt(a, b):
    return lax.dot_general(a, b, (((1,), (1,)), ((), ())), preferred_element_type=F32)


def dot_tn(a, b):
    return lax.dot_general(a, b, (((0,), (0,)), ((), ())), preferred_element_type=F32)


def call(kernel, grid, in_specs, out_specs, out_shape, flops, nbytes, scratch=(), prefetch=0, trans=0):
    return pl.pallas_call(
        kernel,
        grid_spec=pltpu.PrefetchScalarGridSpec(
            num_scalar_prefetch=prefetch, grid=grid, in_specs=in_specs, out_specs=out_specs, scratch_shapes=list(scratch)),
        out_shape=out_shape,
        cost_estimate=pl.CostEstimate(flops=flops, bytes_accessed=nbytes, transcendentals=trans),
        compiler_params=pltpu.CompilerParams(vmem_limit_bytes=VMEM_LIMIT))


def sds(shape, dtype):
    return jax.ShapeDtypeStruct(shape, dtype)


def norm_blocks(stream, gain, order_x, order_y):
    tokens, width = stream.shape
    block = width // 8

    def kernel(ox_ref, oy_ref, x_ref, g_ref, n_ref, nx_ref, ny_ref):
        hat, _ = width_norm(x_ref[...])
        n_ref[...] = (hat * g_ref[...]).astype(BF16)
        for j in range(8):
            cols = slice(j * block, (j + 1) * block)
            nx_ref[:, cols] = n_ref[:, pl.ds(pl.multiple_of(ox_ref[j] * block, block), block)]
            ny_ref[:, cols] = n_ref[:, pl.ds(pl.multiple_of(oy_ref[j] * block, block), block)]

    whole = pl.BlockSpec((tokens, width), lambda i, ox, oy: (0, 0))
    return call(kernel, (1,), [whole, pl.BlockSpec((1, width), lambda i, ox, oy: (0, 0))], [whole] * 3,
                [sds((tokens, width), BF16)] * 3, 10 * tokens * width, 8 * tokens * width,
                prefetch=2)(order_x, order_y, stream, gain[None])


def project(values, weights, column, width, tile=512):
    tokens, depth = values.shape
    first = column // tile

    def kernel(x_ref, w_ref, o_ref):
        o_ref[...] = dot_nn(x_ref[...], w_ref[...])

    return call(kernel, (width // tile,),
                [pl.BlockSpec((tokens, depth), lambda j: (0, 0)),
                 pl.BlockSpec((depth, tile), lambda j: (0, first + j))],
                pl.BlockSpec((tokens, tile), lambda j: (0, j)),
                sds((tokens, width), F32), 2 * tokens * depth * width,
                2 * depth * width + 4 * tokens * width)(values, weights)


def swiglu_forward(values, weights, column, width, place_x, place_y):
    tokens, depth = values.shape
    tile = width // 8
    first = column // tile

    def kernel(px_ref, py_ref, x_ref, wg_ref, wu_ref, g_ref, u_ref, m_ref, mx_ref, my_ref):
        x = x_ref[...]
        gate = dot_nn(x, wg_ref[...])
        up = dot_nn(x, wu_ref[...])
        g_ref[...] = gate
        u_ref[...] = up
        hidden = (gate * jax.nn.sigmoid(gate) * up).astype(BF16)
        m_ref[...] = hidden
        mx_ref[...] = hidden
        my_ref[...] = hidden

    col = pl.BlockSpec((tokens, tile), lambda j, px, py: (0, j))
    return call(kernel, (8,),
                [pl.BlockSpec((tokens, depth), lambda j, px, py: (0, 0)),
                 pl.BlockSpec((depth, tile), lambda j, px, py: (0, first + j)),
                 pl.BlockSpec((depth, tile), lambda j, px, py: (0, first + 8 + j))],
                [col, col, col, pl.BlockSpec((tokens, tile), lambda j, px, py: (0, px[j])),
                 pl.BlockSpec((tokens, tile), lambda j, px, py: (0, py[j]))],
                [sds((tokens, width), F32)] * 2 + [sds((tokens, width), BF16)] * 3,
                4 * tokens * depth * width, 4 * depth * width + 14 * tokens * width,
                trans=tokens * width, prefetch=2)(place_x, place_y, values, weights, weights)


def output_projection(stream, attn, hidden, weights, tile=256):
    tokens, model = stream.shape
    parts, rows, _ = weights.shape
    attn_w, hid_w = attn.shape[1], hidden.shape[1]
    attn_rows = attn_w // parts

    def kernel(x_ref, a_ref, m_ref, w_ref, y_ref):
        w_o = w_ref[:, :attn_rows, :].reshape(attn_w, tile)
        w_d = w_ref[:, attn_rows:, :].reshape(hid_w, tile)
        total = x_ref[...].astype(F32) + dot_nn(a_ref[...], w_o) + dot_nn(m_ref[...], w_d)
        y_ref[...] = total.astype(BF16)

    col = pl.BlockSpec((tokens, tile), lambda j: (0, j))
    return call(kernel, (model // tile,),
                [col, pl.BlockSpec((tokens, attn_w), lambda j: (0, 0)),
                 pl.BlockSpec((tokens, hid_w), lambda j: (0, 0)),
                 pl.BlockSpec((parts, rows, tile), lambda j: (0, 0, j))],
                col, sds((tokens, model), BF16), 2 * tokens * model * (attn_w + hid_w),
                2 * (attn_w + hid_w) * (model + tokens))(stream, attn, hidden, weights)


def output_backward(grad_y, weights, gate, up, attn_w):
    tokens, model = grad_y.shape
    parts, rows, _ = weights.shape
    hid_w = gate.shape[1]
    ar, hr = attn_w // parts, hid_w // parts

    def kernel(gy_ref, w_ref, g_ref, u_ref, da_ref, dg_ref, du_ref):
        gy = gy_ref[...]
        da_ref[...] = dot_nt(gy, w_ref[0, :ar, :]).astype(BF16)
        d_hidden = dot_nt(gy, w_ref[0, ar:, :])
        gate_v = g_ref[...]
        sig = jax.nn.sigmoid(gate_v)
        silu = gate_v * sig
        du_ref[...] = (d_hidden * silu).astype(BF16)
        dg_ref[...] = (d_hidden * u_ref[...] * (sig + silu * (1.0 - sig))).astype(BF16)

    def col(width):
        return pl.BlockSpec((tokens, width), lambda j: (0, j))

    return call(kernel, (parts,),
                [pl.BlockSpec((tokens, model), lambda j: (0, 0)),
                 pl.BlockSpec((1, rows, model), lambda j: (j, 0, 0)), col(hr), col(hr)],
                [col(ar), col(hr), col(hr)],
                [sds((tokens, attn_w), BF16), sds((tokens, hid_w), BF16), sds((tokens, hid_w), BF16)],
                2 * tokens * model * (attn_w + hid_w),
                2 * (attn_w + hid_w) * model + 12 * tokens * hid_w + 2 * tokens * attn_w,
                trans=tokens * hid_w)(grad_y, weights, gate, up)


def input_backward(pieces, tile=512):
    tokens = pieces[0][0].shape[0]
    depth = pieces[0][1].shape[0]
    total = None
    for grads, weights, column in pieces:
        steps = grads.shape[1] // tile
        first = column // tile
        has_total = total is not None

        def kernel(*refs, steps=steps, has_total=has_total):
            d_ref, w_ref = refs[0], refs[1]
            o_ref = refs[-1]
            part = dot_nt(d_ref[...], w_ref[...])

            @pl.when(pl.program_id(0) == 0)
            def _():
                o_ref[...] = part + refs[2][...] if has_total else part

            @pl.when(pl.program_id(0) > 0)
            def _():
                o_ref[...] += part

        whole = pl.BlockSpec((tokens, depth), lambda j: (0, 0))
        specs = [pl.BlockSpec((tokens, tile), lambda j: (0, j)),
                 pl.BlockSpec((depth, tile), lambda j, first=first: (0, first + j))]
        args = [grads, weights]
        if has_total:
            specs.append(whole)
            args.append(total)
        total = call(kernel, (steps,), specs, whole, sds((tokens, depth), F32),
                     2 * tokens * depth * tile * steps, 2 * (tokens + depth) * tile * steps + 4 * tokens * depth)(*args)
    return total


def swap_pairs(values):
    lane = lax.broadcasted_iota(jnp.int32, values.shape, 1)
    return jnp.where(lane % 2 == 0, pltpu.roll(values, HEAD_DIM - 1, 1), pltpu.roll(values, 1, 1))


def head_norm(values):
    mean = jnp.mean(values, axis=-1, keepdims=True)
    centered = values - mean
    rstd = lax.rsqrt(jnp.mean(centered * centered, axis=-1, keepdims=True) + EPSILON)
    return centered * rstd, rstd


def rope(values, cos, sin):
    return values * cos + swap_pairs(values) * sin


def scores_t(k, q, start):
    keys = lax.broadcasted_iota(jnp.int32, (k.shape[0], q.shape[0]), 0)
    queries = lax.broadcasted_iota(jnp.int32, (k.shape[0], q.shape[0]), 1) + start
    s = jnp.where(queries >= keys, dot_nt(k, q) * HEAD_DIM ** -0.5, -1e30)
    e = jnp.exp(s - jnp.max(s, axis=0, keepdims=True))
    return e * (1.0 / jnp.sum(e, axis=0, keepdims=True))


def attention_specs(tokens):
    table = pl.BlockSpec((tokens, HEAD_DIM), lambda h, *_: (0, 0))
    return [pl.BlockSpec((tokens, 512), lambda h, *_: (0, h)),
            pl.BlockSpec((1, 2, HEAD_DIM), lambda h, *_: (h, 0, 0)),
            pl.BlockSpec((1, 1, HEAD_DIM), lambda h, *_: (h, 0, 0)), table, table]


def attention_forward(qkv, q_norm, k_norm, cos, sin, place, block=256):
    tokens = qkv.shape[0]
    groups = qkv.shape[1] // 512

    def kernel(place_ref, qkv_ref, qn_ref, kn_ref, cos_ref, sin_ref, o_ref, op_ref):
        cos_v, sin_v = cos_ref[...], sin_ref[...]
        k = rope(head_norm(qkv_ref[:, 256:384])[0] * kn_ref[0], cos_v, sin_v).astype(BF16)
        v_t = qkv_ref[:, 384:512].T.astype(BF16)
        for head in range(2):
            cols = slice(head * HEAD_DIM, (head + 1) * HEAD_DIM)
            q = rope(head_norm(qkv_ref[:, cols])[0] * qn_ref[0, head:head + 1, :], cos_v, sin_v).astype(BF16)
            for start in range(0, tokens, block):
                stop = start + block
                prob = scores_t(k[:stop], q[start:stop], start).astype(BF16)
                out = dot_nn(v_t[:, :stop], prob).T.astype(BF16)
                o_ref[start:stop, cols] = out
                op_ref[start:stop, cols] = out

    return call(kernel, (groups,), attention_specs(tokens),
                [pl.BlockSpec((tokens, 256), lambda h, p: (0, h)), pl.BlockSpec((tokens, 256), lambda h, p: (0, p[h]))],
                [sds((tokens, groups * 256), BF16)] * 2,
                groups * 2 * 4 * tokens * tokens * HEAD_DIM, 4 * tokens * groups * 512 + 4 * tokens * groups * 256,
                trans=groups * 2 * tokens * tokens, prefetch=1)(place, qkv, q_norm, k_norm, cos, sin)


def attention_backward(qkv, d_attn, q_norm, k_norm, cos, sin, block=256):
    tokens = qkv.shape[0]
    groups = qkv.shape[1] // 512

    def norm_back(d_rot, hat, rstd, gain, cos_v, sin_v):
        d_rot = d_rot.astype(BF16).astype(F32)
        d_out = d_rot * cos_v - swap_pairs(d_rot) * sin_v
        d_gain = jnp.sum(d_out * hat, axis=0, keepdims=True)
        d_hat = d_out * gain
        d_in = rstd * (d_hat - jnp.mean(d_hat, axis=-1, keepdims=True)
                       - hat * jnp.mean(d_hat * hat, axis=-1, keepdims=True))
        return d_in.astype(BF16), d_gain

    def kernel(qkv_ref, qn_ref, kn_ref, cos_ref, sin_ref, do_ref, d_ref, gq_ref, gk_ref, dk_acc, dv_acc, dq_acc):
        cos_v, sin_v = cos_ref[...], sin_ref[...]
        k_hat, k_rstd = head_norm(qkv_ref[:, 256:384])
        k_rot = rope(k_hat * kn_ref[0], cos_v, sin_v)
        k = k_rot.astype(BF16)
        k_t = k_rot.T.astype(BF16)
        v = qkv_ref[:, 384:512].astype(BF16)
        dk_acc[...] = jnp.zeros_like(dk_acc)
        dv_acc[...] = jnp.zeros_like(dv_acc)
        for head in range(2):
            cols = slice(head * HEAD_DIM, (head + 1) * HEAD_DIM)
            q_hat, q_rstd = head_norm(qkv_ref[:, cols])
            q = rope(q_hat * qn_ref[0, head:head + 1, :], cos_v, sin_v).astype(BF16)
            for start in range(0, tokens, block):
                stop = start + block
                q_b = q[start:stop]
                do_b = do_ref[start:stop, cols]
                prob = scores_t(k[:stop], q_b, start)
                dv_acc[:stop] += dot_nn(prob.astype(BF16), do_b)
                d_prob = dot_nt(v[:stop], do_b).astype(BF16).astype(F32)
                weighted = prob * d_prob
                d_s = weighted - prob * jnp.sum(weighted, axis=0, keepdims=True)
                d_s = (d_s * HEAD_DIM ** -0.5).astype(BF16)
                dk_acc[:stop] += dot_nn(d_s, q_b)
                dq_acc[start:stop, :] = dot_nn(k_t[:, :stop], d_s).T
            d_in, d_gain = norm_back(dq_acc[...], q_hat, q_rstd, qn_ref[0, head:head + 1, :], cos_v, sin_v)
            d_ref[:, cols] = d_in
            gq_ref[0, head:head + 1, :] = d_gain
        d_in, d_gain = norm_back(dk_acc[...], k_hat, k_rstd, kn_ref[0], cos_v, sin_v)
        d_ref[:, 256:384] = d_in
        gk_ref[0] = d_gain
        d_ref[:, 384:512] = dv_acc[...].astype(BF16)

    return call(kernel, (groups,),
                attention_specs(tokens) + [pl.BlockSpec((tokens, 256), lambda h: (0, h))],
                [pl.BlockSpec((tokens, 512), lambda h: (0, h)),
                 pl.BlockSpec((1, 2, HEAD_DIM), lambda h: (h, 0, 0)),
                 pl.BlockSpec((1, 1, HEAD_DIM), lambda h: (h, 0, 0))],
                [sds((tokens, groups * 512), BF16), sds((groups, 2, HEAD_DIM), F32), sds((groups, 1, HEAD_DIM), F32)],
                groups * 2 * 10 * tokens * tokens * HEAD_DIM, 6 * tokens * groups * 512 + 2 * tokens * groups * 256,
                scratch=[pltpu.VMEM((tokens, HEAD_DIM), F32)] * 3,
                trans=groups * 2 * tokens * tokens)(qkv, q_norm, k_norm, cos, sin, d_attn)


def width_norm(stream):
    values = stream.astype(F32)
    centered = values - jnp.mean(values, axis=-1, keepdims=True)
    rstd = lax.rsqrt(jnp.mean(centered * centered, axis=-1, keepdims=True) + EPSILON)
    return centered * rstd, rstd


def width_norm_backward(stream, gain, d_normed):
    hat, rstd = width_norm(stream)
    d_gain = jnp.sum(d_normed * hat, axis=0)
    d_hat = d_normed * gain
    d_in = rstd * (d_hat - jnp.mean(d_hat, axis=-1, keepdims=True)
                   - hat * jnp.mean(d_hat * hat, axis=-1, keepdims=True))
    return d_in, d_gain


def exchange(values, bit):
    return lax.ppermute(values, AXIS, [(i, i ^ bit) for i in range(8)])


def reduce_product(acts, cotangent, x_first):
    rows = acts.shape[1] // 8
    first, second = (X_BIT, Y_BIT) if x_first else (Y_BIT, X_BIT)
    odd = dot_tn(acts[:, :4 * rows], cotangent)
    from_core = exchange(odd, CORE_BIT)
    sent = dot_tn(acts[:, 4 * rows:6 * rows], cotangent) + from_core[:2 * rows]
    from_first = exchange(sent, first)
    kept = dot_tn(acts[:, 6 * rows:], cotangent) + from_core[2 * rows:]
    passed = kept[rows:] + from_first[rows:]
    from_second = exchange(passed, second)
    return kept[:rows] + from_first[:rows] + from_second


def reduce_vector(values):
    me = lax.axis_index(AXIS)
    blocks = values[jnp.array(ORDER_X_FIRST) ^ me]
    from_core = exchange(blocks[:4], CORE_BIT)
    kept = blocks[4:] + from_core
    from_x = exchange(kept[:2], X_BIT)
    kept = kept[2:] + from_x
    return kept[0] + exchange(kept[1], Y_BIT)


def gather(shard):
    return lax.all_gather(shard, AXIS, axis=0, tiled=True)


def solution(mesh):
    act_spec = P(AXIS, None, None)
    vec, mat = P(AXIS), P(AXIS, None)
    param_spec = (vec,) + (mat,) * 7 + (vec, vec)
    in_specs = (act_spec, P(), act_spec) + param_spec + param_spec
    out_specs = (act_spec, act_spec) + param_spec + param_spec

    def body(x_in, positions, grad_out, *shards):
        me = lax.axis_index(AXIS)
        lanes = jnp.arange(8, dtype=jnp.int32)
        order_x = jnp.array(ORDER_X_FIRST, jnp.int32) ^ me
        order_y = jnp.array(ORDER_Y_FIRST, jnp.int32) ^ me
        place_x = jnp.array([ORDER_X_FIRST.index(i) for i in range(8)], jnp.int32)[lanes ^ me]
        place_y = jnp.array([ORDER_Y_FIRST.index(i) for i in range(8)], jnp.int32)[lanes ^ me]
        layers = (shards[:10], shards[10:])

        def in_shard(p):
            rows = p[1].shape[0]
            parts = [p[1].reshape(rows, 8, 256), p[2].reshape(rows, 8, 128), p[3].reshape(rows, 8, 128)]
            qkv = jnp.concatenate(parts, axis=2).reshape(rows, 4096)
            return jnp.concatenate([p[5], p[6], qkv], axis=1)

        def out_shard(p):
            return jnp.concatenate([p[4], p[7]], axis=0)[None]

        one, two = layers
        vectors = gather(jnp.concatenate([one[0], one[8], one[9], two[0], two[8], two[9]])[None])
        w_in, w_out = [], []
        for p in layers:
            w_in.append(gather(in_shard(p)))
            w_out.append(gather(out_shard(p)))
        gains = []
        for base in (0, 512):
            gains.append((vectors[:, base:base + 128].reshape(-1),
                          vectors[:, base + 128:base + 384].reshape(8, 2, 128),
                          vectors[:, base + 384:base + 512].reshape(8, 1, 128)))

        inv_freq = ROPE_THETA ** (-jnp.arange(0, HEAD_DIM, 2, dtype=F32) / HEAD_DIM)
        angles = positions.astype(F32)[:, None] * jnp.repeat(inv_freq, 2)[None, :]
        cos = jnp.cos(angles)
        sin = jnp.sin(angles) * jnp.where(jnp.arange(HEAD_DIM) % 2 == 0, -1.0, 1.0)[None, :]

        stream = x_in[0]
        saved = []
        for index in range(2):
            ln_gain, q_gain, k_gain = gains[index]
            normed, normed_x, normed_y = norm_blocks(stream, ln_gain, order_x, order_y)
            qkv = project(normed, w_in[index], 6144, 4096)
            gate, up, *hidden = swiglu_forward(normed, w_in[index], 0, 3072, place_x, place_y)
            attn = attention_forward(qkv, q_gain, k_gain, cos, sin, place_x if index else place_y)
            saved.append((stream, normed_x, normed_y, qkv, attn[1], gate, up, hidden))
            stream = output_projection(stream, attn[0], hidden[0], w_out[index])
        y_out = stream

        grad = grad_out[0]
        results = [None, None]
        for index in (1, 0):
            ln_gain, q_gain, k_gain = gains[index]
            stream, normed_x, normed_y, qkv, attn, gate, up, hidden = saved[index]
            g_down = jnp.concatenate([reduce_product(hidden[1], grad[:, :512], True),
                                      reduce_product(hidden[2], grad[:, 512:], False)], axis=1)
            d_attn, d_gate, d_up = output_backward(grad, w_out[index], gate, up, attn.shape[1])
            g_gate = reduce_product(normed_x, d_gate, True)
            g_up = reduce_product(normed_y, d_up, False)
            g_o = reduce_product(attn, grad, index == 1)
            d_qkv, g_qn, g_kn = attention_backward(qkv, d_attn, q_gain, k_gain, cos, sin)
            g_qkv = jnp.concatenate([reduce_product(normed_x, d_qkv[:, :2048], True),
                                     reduce_product(normed_y, d_qkv[:, 2048:], False)], axis=1)
            d_normed = input_backward([(d_gate, w_in[index], 0), (d_up, w_in[index], 3072),
                                       (d_qkv, w_in[index], 6144)])
            d_stream, g_ln = width_norm_backward(stream, ln_gain, d_normed)
            grad = (grad.astype(F32) + d_stream).astype(BF16)
            g_vec = reduce_vector(jnp.concatenate(
                [g_ln.reshape(8, 128), g_qn.reshape(8, 256), g_kn.reshape(8, 128)], axis=1))
            split = g_qkv.reshape(128, 8, 512)
            results[index] = (g_vec[:128], split[:, :, :256].reshape(128, 2048), split[:, :, 256:384].reshape(128, 1024),
                              split[:, :, 384:].reshape(128, 1024), g_o, g_gate, g_up, g_down,
                              g_vec[128:384], g_vec[384:])
        return (y_out[None], grad[None]) + results[0] + results[1]

    return jax.shard_map(body, mesh=mesh, in_specs=in_specs, out_specs=out_specs, check_vma=False)
```

```python
import jax
import jax.numpy as jnp
from jax import lax
from jax.experimental import pallas as pl
from jax.experimental.pallas import tpu as pltpu
from jax.sharding import PartitionSpec as P


HEAD_DIM = 128
EPSILON = 1e-5
ROPE_THETA = 7.5e7
AXIS = 'fsdp'
F32 = jnp.float32
BF16 = jnp.bfloat16
VMEM_LIMIT = 60 * 1024 * 1024
CORE_BIT, X_BIT, Y_BIT = 1, 2, 4
ORDER_X_FIRST = (3, 7, 1, 5, 2, 6, 0, 4)
ORDER_Y_FIRST = (5, 7, 1, 3, 4, 6, 0, 2)


def dot_nn(a, b):
    return lax.dot_general(a, b, (((1,), (0,)), ((), ())), preferred_element_type=F32)


def dot_nt(a, b):
    return lax.dot_general(a, b, (((1,), (1,)), ((), ())), preferred_element_type=F32)


def dot_tn(a, b):
    return lax.dot_general(a, b, (((0,), (0,)), ((), ())), preferred_element_type=F32)


def call(kernel, grid, in_specs, out_specs, out_shape, flops, nbytes, scratch=(), prefetch=0, trans=0):
    return pl.pallas_call(
        kernel,
        grid_spec=pltpu.PrefetchScalarGridSpec(
            num_scalar_prefetch=prefetch, grid=grid, in_specs=in_specs, out_specs=out_specs, scratch_shapes=list(scratch)),
        out_shape=out_shape,
        cost_estimate=pl.CostEstimate(flops=flops, bytes_accessed=nbytes, transcendentals=trans),
        compiler_params=pltpu.CompilerParams(vmem_limit_bytes=VMEM_LIMIT))


def sds(shape, dtype):
    return jax.ShapeDtypeStruct(shape, dtype)


def norm_blocks(stream, gain, order_x, order_y):
    tokens, width = stream.shape
    block = width // 8

    def kernel(ox_ref, oy_ref, x_ref, g_ref, n_ref, nx_ref, ny_ref):
        hat, _ = width_norm(x_ref[...])
        n_ref[...] = (hat * g_ref[...]).astype(BF16)
        for j in range(8):
            cols = slice(j * block, (j + 1) * block)
            nx_ref[:, cols] = n_ref[:, pl.ds(pl.multiple_of(ox_ref[j] * block, block), block)]
            ny_ref[:, cols] = n_ref[:, pl.ds(pl.multiple_of(oy_ref[j] * block, block), block)]

    whole = pl.BlockSpec((tokens, width), lambda i, ox, oy: (0, 0))
    return call(kernel, (1,), [whole, pl.BlockSpec((1, width), lambda i, ox, oy: (0, 0))], [whole] * 3,
                [sds((tokens, width), BF16)] * 3, 10 * tokens * width, 8 * tokens * width,
                prefetch=2)(order_x, order_y, stream, gain[None])


def swiglu_forward(values, weights, column, width, place_x, place_y):
    tokens, depth = values.shape
    tile = width // 8
    first = column // tile

    def kernel(px_ref, py_ref, x_ref, wg_ref, wu_ref, g_ref, u_ref, m_ref, mx_ref, my_ref):
        x = x_ref[...]
        gate = dot_nn(x, wg_ref[...])
        up = dot_nn(x, wu_ref[...])
        g_ref[...] = gate
        u_ref[...] = up
        hidden = (gate * jax.nn.sigmoid(gate) * up).astype(BF16)
        m_ref[...] = hidden
        mx_ref[...] = hidden
        my_ref[...] = hidden

    col = pl.BlockSpec((tokens, tile), lambda j, px, py: (0, j))
    return call(kernel, (8,),
                [pl.BlockSpec((tokens, depth), lambda j, px, py: (0, 0)),
                 pl.BlockSpec((depth, tile), lambda j, px, py: (0, first + j)),
                 pl.BlockSpec((depth, tile), lambda j, px, py: (0, first + 8 + j))],
                [col, col, col, pl.BlockSpec((tokens, tile), lambda j, px, py: (0, px[j])),
                 pl.BlockSpec((tokens, tile), lambda j, px, py: (0, py[j]))],
                [sds((tokens, width), F32)] * 2 + [sds((tokens, width), BF16)] * 3,
                4 * tokens * depth * width, 4 * depth * width + 14 * tokens * width,
                trans=tokens * width, prefetch=2)(place_x, place_y, values, weights, weights)


def output_projection(stream, attn, hidden, weights, tile=256):
    tokens, model = stream.shape
    parts, rows, _ = weights.shape
    attn_w, hid_w = attn.shape[1], hidden.shape[1]
    attn_rows = attn_w // parts

    def kernel(x_ref, a_ref, m_ref, w_ref, y_ref):
        w_o = w_ref[:, :attn_rows, :].reshape(attn_w, tile)
        w_d = w_ref[:, attn_rows:, :].reshape(hid_w, tile)
        total = x_ref[...].astype(F32) + dot_nn(a_ref[...], w_o) + dot_nn(m_ref[...], w_d)
        y_ref[...] = total.astype(BF16)

    col = pl.BlockSpec((tokens, tile), lambda j: (0, j))
    return call(kernel, (model // tile,),
                [col, pl.BlockSpec((tokens, attn_w), lambda j: (0, 0)),
                 pl.BlockSpec((tokens, hid_w), lambda j: (0, 0)),
                 pl.BlockSpec((parts, rows, tile), lambda j: (0, 0, j))],
                col, sds((tokens, model), BF16), 2 * tokens * model * (attn_w + hid_w),
                2 * (attn_w + hid_w) * (model + tokens))(stream, attn, hidden, weights)


def output_backward(grad_y, weights, gate, up, attn_w):
    tokens, model = grad_y.shape
    parts, rows, _ = weights.shape
    hid_w = gate.shape[1]
    ar, hr = attn_w // parts, hid_w // parts

    def kernel(gy_ref, w_ref, g_ref, u_ref, da_ref, dg_ref, du_ref):
        gy = gy_ref[...]
        da_ref[...] = dot_nt(gy, w_ref[0, :ar, :]).astype(BF16)
        d_hidden = dot_nt(gy, w_ref[0, ar:, :])
        gate_v = g_ref[...]
        sig = jax.nn.sigmoid(gate_v)
        silu = gate_v * sig
        du_ref[...] = (d_hidden * silu).astype(BF16)
        dg_ref[...] = (d_hidden * u_ref[...] * (sig + silu * (1.0 - sig))).astype(BF16)

    def col(width):
        return pl.BlockSpec((tokens, width), lambda j: (0, j))

    return call(kernel, (parts,),
                [pl.BlockSpec((tokens, model), lambda j: (0, 0)),
                 pl.BlockSpec((1, rows, model), lambda j: (j, 0, 0)), col(hr), col(hr)],
                [col(ar), col(hr), col(hr)],
                [sds((tokens, attn_w), BF16), sds((tokens, hid_w), BF16), sds((tokens, hid_w), BF16)],
                2 * tokens * model * (attn_w + hid_w),
                2 * (attn_w + hid_w) * model + 12 * tokens * hid_w + 2 * tokens * attn_w,
                trans=tokens * hid_w)(grad_y, weights, gate, up)


def input_backward(d_gate, d_up, d_qkv_a, d_qkv_b, w_gu, w_qkv, qkv_column, stream, gain, grad_y, tile=1024):
    tokens, depth = stream.shape
    gate_steps = d_gate.shape[1] // tile
    gu_steps = 2 * gate_steps
    half_steps = d_qkv_a.shape[1] // tile
    a_steps = gu_steps + half_steps
    first = qkv_column // tile
    steps = a_steps + half_steps

    def kernel(dg_ref, du_ref, da_ref, db_ref, wa_ref, wb_ref, x_ref, gain_ref, gy_ref, gx_ref, gg_ref, acc):
        j = pl.program_id(0)

        @pl.when(j == 0)
        def _():
            acc[...] = dot_nt(dg_ref[...], wa_ref[...])

        @pl.when((j > 0) & (j < gate_steps))
        def _():
            acc[...] += dot_nt(dg_ref[...], wa_ref[...])

        @pl.when((j >= gate_steps) & (j < gu_steps))
        def _():
            acc[...] += dot_nt(du_ref[...], wa_ref[...])

        @pl.when((j >= gu_steps) & (j < a_steps))
        def _():
            acc[...] += dot_nt(da_ref[...], wb_ref[...])

        @pl.when(j >= a_steps)
        def _():
            acc[...] += dot_nt(db_ref[...], wb_ref[...])

        @pl.when(j == steps - 1)
        def _():
            hat, rstd = width_norm(x_ref[...])
            d_normed = acc[...]
            gg_ref[...] = jnp.sum(d_normed * hat, axis=0, keepdims=True)
            d_hat = d_normed * gain_ref[...]
            d_in = rstd * (d_hat - jnp.mean(d_hat, axis=-1, keepdims=True)
                           - hat * jnp.mean(d_hat * hat, axis=-1, keepdims=True))
            gx_ref[...] = (gy_ref[...].astype(F32) + d_in).astype(BF16)

    whole = pl.BlockSpec((tokens, depth), lambda j: (0, 0))
    row = pl.BlockSpec((1, depth), lambda j: (0, 0))
    return call(kernel, (steps,),
                [pl.BlockSpec((tokens, tile), lambda j: (0, jnp.minimum(j, gate_steps - 1))),
                 pl.BlockSpec((tokens, tile), lambda j: (0, jnp.clip(j - gate_steps, 0, gate_steps - 1))),
                 pl.BlockSpec((tokens, tile), lambda j: (0, jnp.clip(j - gu_steps, 0, half_steps - 1))),
                 pl.BlockSpec((tokens, tile), lambda j: (0, jnp.clip(j - a_steps, 0, half_steps - 1))),
                 pl.BlockSpec((depth, tile), lambda j: (0, jnp.minimum(j, gu_steps - 1))),
                 pl.BlockSpec((depth, tile), lambda j: (0, first + jnp.maximum(j - gu_steps, 0))),
                 whole, row, whole],
                [whole, row], [sds((tokens, depth), BF16), sds((1, depth), F32)],
                2 * tokens * depth * tile * steps, 2 * (tokens + depth) * tile * steps + 6 * tokens * depth,
                scratch=[pltpu.VMEM((tokens, depth), F32)])(
                    d_gate, d_up, d_qkv_a, d_qkv_b, w_gu, w_qkv, stream, gain[None], grad_y)


def swap_pairs(values):
    lane = lax.broadcasted_iota(jnp.int32, values.shape, 1)
    return jnp.where(lane % 2 == 0, pltpu.roll(values, HEAD_DIM - 1, 1), pltpu.roll(values, 1, 1))


def head_norm(values):
    mean = jnp.mean(values, axis=-1, keepdims=True)
    centered = values - mean
    rstd = lax.rsqrt(jnp.mean(centered * centered, axis=-1, keepdims=True) + EPSILON)
    return centered * rstd, rstd


def rope(values, cos, sin):
    return values * cos + swap_pairs(values) * sin


SCALE = HEAD_DIM ** -0.5
SCALE_LOG2E = SCALE * 1.4426950408889634


def causal_block(block):
    keys = lax.broadcasted_iota(jnp.int32, (block, 2 * block), 0)
    queries = lax.broadcasted_iota(jnp.int32, (block, 2 * block), 1) % block
    return queries >= keys


def head_specs(first=0):
    return [pl.BlockSpec((1, 2, HEAD_DIM), lambda h, *_: (first + h, 0, 0)),
            pl.BlockSpec((1, 1, HEAD_DIM), lambda h, *_: (first + h, 0, 0))]


def attention_forward(normed, weights, column, q_norm, k_norm, cos, sin, place, block=256):
    tokens, depth = normed.shape
    groups = q_norm.shape[0]
    first = column // 512
    blocks = tokens // block

    def kernel(place_ref, x_ref, w_ref, qn_ref, kn_ref, cos_ref, sin_ref, raw_ref, rot_ref, lse_ref, o_ref, op_ref):
        cos_v, sin_v = cos_ref[...], sin_ref[...]
        raw = dot_nn(x_ref[...], w_ref[...])
        raw_ref[...] = raw[:, :384]
        for part, gain in enumerate((qn_ref[0, 0:1, :], qn_ref[0, 1:2, :], kn_ref[0])):
            cols = slice(part * HEAD_DIM, (part + 1) * HEAD_DIM)
            rot_ref[:, cols] = rope(head_norm(raw_ref[:, cols])[0] * gain, cos_v, sin_v).astype(BF16)
        rot_ref[:, 384:512] = raw[:, 384:].astype(BF16)
        v_t = raw[:, 384:].T.astype(BF16)
        mask = causal_block(block)
        for index in range(blocks):
            start, stop = index * block, (index + 1) * block
            q = jnp.concatenate([rot_ref[start:stop, :128], rot_ref[start:stop, 128:256]], axis=0)
            s = dot_nt(rot_ref[:stop, 256:384], q)
            diag = jnp.where(mask, s[start:], -1e30)
            s = jnp.concatenate([s[:start], diag], axis=0) if index else diag
            top = jnp.max(s, axis=0, keepdims=True)
            e = jnp.exp2((s - top) * SCALE_LOG2E)
            total = jnp.sum(e, axis=0, keepdims=True)
            lse_ref[0, index:index + 1, :] = top * SCALE_LOG2E + jnp.log2(total)
            out = dot_nn(v_t[:, :stop], (e * (1.0 / total)).astype(BF16))
            for head in range(2):
                value = out[:, head * block:(head + 1) * block].T.astype(BF16)
                o_ref[start:stop, head * HEAD_DIM:(head + 1) * HEAD_DIM] = value
                op_ref[start:stop, head * HEAD_DIM:(head + 1) * HEAD_DIM] = value

    table = pl.BlockSpec((tokens, HEAD_DIM), lambda h, p: (0, 0))

    def col(width):
        return pl.BlockSpec((tokens, width), lambda h, p: (0, h))

    return call(kernel, (groups,),
                [pl.BlockSpec((tokens, depth), lambda h, p: (0, 0)),
                 pl.BlockSpec((depth, 512), lambda h, p: (0, first + h))] + head_specs() + [table, table],
                [col(384), col(512), pl.BlockSpec((1, blocks, 2 * block), lambda h, p: (h, 0, 0)), col(256),
                 pl.BlockSpec((tokens, 256), lambda h, p: (0, p[h]))],
                [sds((tokens, groups * 384), F32), sds((tokens, groups * 512), BF16), sds((groups, blocks, 2 * block), F32),
                 sds((tokens, groups * 256), BF16), sds((tokens, groups * 256), BF16)],
                groups * 2 * 4 * tokens * tokens * HEAD_DIM + 2 * tokens * depth * groups * 512,
                2 * depth * groups * 512 + tokens * groups * (384 * 4 + 512 * 2 + 512 * 2),
                trans=groups * 2 * tokens * tokens, prefetch=1)(place, normed, weights, q_norm, k_norm, cos, sin)


def attention_backward(raw, rot, lse, d_attn, q_norm, k_norm, cos, sin, first, groups, block=256):
    tokens = raw.shape[0]
    blocks = tokens // block

    def norm_back(d_rot, values, gain, cos_v, sin_v):
        hat, rstd = head_norm(values)
        d_rot = d_rot.astype(BF16).astype(F32)
        d_out = d_rot * cos_v - swap_pairs(d_rot) * sin_v
        d_gain = jnp.sum(d_out * hat, axis=0, keepdims=True)
        d_hat = d_out * gain
        d_in = rstd * (d_hat - jnp.mean(d_hat, axis=-1, keepdims=True)
                       - hat * jnp.mean(d_hat * hat, axis=-1, keepdims=True))
        return d_in.astype(BF16), d_gain

    def kernel(raw_ref, rot_ref, lse_ref, do_ref, qn_ref, kn_ref, cos_ref, sin_ref, d_ref, gq_ref, gk_ref,
               dk_acc, dv_acc, dq_acc):
        k_t = rot_ref[:, 256:384].astype(F32).T.astype(BF16)
        mask = causal_block(block)
        for index in reversed(range(blocks)):
            start, stop = index * block, (index + 1) * block
            q = jnp.concatenate([rot_ref[start:stop, :128], rot_ref[start:stop, 128:256]], axis=0)
            d_o = jnp.concatenate([do_ref[start:stop, :128], do_ref[start:stop, 128:256]], axis=0)
            s = dot_nt(rot_ref[:stop, 256:384], q)
            prob = jnp.exp2(s * SCALE_LOG2E - lse_ref[0, index:index + 1, :])
            diag = jnp.where(mask, prob[start:], 0.0)
            prob = jnp.concatenate([prob[:start], diag], axis=0) if index else diag
            d_v = dot_nn(prob.astype(BF16), d_o)
            d_prob = dot_nt(rot_ref[:stop, 384:512], d_o).astype(BF16).astype(F32)
            delta = jnp.sum(prob * d_prob, axis=0, keepdims=True)
            d_s = (prob * (d_prob - delta) * SCALE).astype(BF16)
            d_k = dot_nn(d_s, q)
            if stop == tokens:
                dv_acc[...] = d_v
                dk_acc[...] = d_k
            else:
                dv_acc[:stop] += d_v
                dk_acc[:stop] += d_k
            d_q = dot_nn(k_t[:, :stop], d_s)
            for head in range(2):
                dq_acc[start:stop, head * HEAD_DIM:(head + 1) * HEAD_DIM] = d_q[:, head * block:(head + 1) * block].T
        cos_v, sin_v = cos_ref[...], sin_ref[...]
        for head in range(2):
            cols = slice(head * HEAD_DIM, (head + 1) * HEAD_DIM)
            d_in, d_gain = norm_back(dq_acc[:, cols], raw_ref[:, cols], qn_ref[0, head:head + 1, :], cos_v, sin_v)
            d_ref[:, cols] = d_in
            gq_ref[0, head:head + 1, :] = d_gain
        d_in, d_gain = norm_back(dk_acc[...], raw_ref[:, 256:384], kn_ref[0], cos_v, sin_v)
        d_ref[:, 256:384] = d_in
        gk_ref[0] = d_gain
        d_ref[:, 384:512] = dv_acc[...].astype(BF16)

    table = pl.BlockSpec((tokens, HEAD_DIM), lambda h: (0, 0))

    def col(width, base=first):
        return pl.BlockSpec((tokens, width), lambda h: (0, base + h))

    return call(kernel, (groups,),
                [col(384), col(512), pl.BlockSpec((1, blocks, 2 * block), lambda h: (first + h, 0, 0)), col(256)]
                + head_specs(first) + [table, table],
                [col(512, 0)] + head_specs(),
                [sds((tokens, groups * 512), BF16), sds((groups, 2, HEAD_DIM), F32), sds((groups, 1, HEAD_DIM), F32)],
                groups * 2 * 10 * tokens * tokens * HEAD_DIM, tokens * groups * (384 * 4 + 512 * 4 + 512),
                scratch=[pltpu.VMEM((tokens, HEAD_DIM), F32), pltpu.VMEM((tokens, HEAD_DIM), F32),
                         pltpu.VMEM((tokens, 2 * HEAD_DIM), F32)],
                trans=groups * 2 * tokens * tokens)(raw, rot, lse, d_attn, q_norm, k_norm, cos, sin)


def width_norm(stream):
    values = stream.astype(F32)
    centered = values - jnp.mean(values, axis=-1, keepdims=True)
    rstd = lax.rsqrt(jnp.mean(centered * centered, axis=-1, keepdims=True) + EPSILON)
    return centered * rstd, rstd


def exchange(values, bit):
    return lax.ppermute(values, AXIS, [(i, i ^ bit) for i in range(8)])


def reduce_product(acts, cotangent, x_first):
    rows = acts.shape[1] // 8
    first, second = (X_BIT, Y_BIT) if x_first else (Y_BIT, X_BIT)
    odd = dot_tn(acts[:, :4 * rows], cotangent)
    from_core = exchange(odd, CORE_BIT)
    sent = dot_tn(acts[:, 4 * rows:6 * rows], cotangent) + from_core[:2 * rows]
    from_first = exchange(sent, first)
    kept = dot_tn(acts[:, 6 * rows:], cotangent) + from_core[2 * rows:]
    passed = kept[rows:] + from_first[rows:]
    from_second = exchange(passed, second)
    return kept[:rows] + from_first[:rows] + from_second


def reduce_vector(values):
    blocks = values[jnp.array(ORDER_X_FIRST) ^ lax.axis_index(AXIS)]
    from_core = exchange(blocks[:4], CORE_BIT)
    kept = blocks[4:] + from_core
    from_first = exchange(kept[:2], X_BIT)
    kept = kept[2:] + from_first
    from_second = exchange(kept[1], Y_BIT)
    return kept[0] + from_second


def gather(shard):
    return lax.all_gather(shard, AXIS, axis=0, tiled=True)


def solution(mesh):
    act_spec = P(AXIS, None, None)
    vec, mat = P(AXIS), P(AXIS, None)
    param_spec = (vec,) + (mat,) * 7 + (vec, vec)
    in_specs = (act_spec, P(), act_spec) + param_spec + param_spec
    out_specs = (act_spec, act_spec) + param_spec + param_spec

    def body(x_in, positions, grad_out, *shards):
        me = lax.axis_index(AXIS)
        lanes = jnp.arange(8, dtype=jnp.int32)
        order_x = jnp.array(ORDER_X_FIRST, jnp.int32) ^ me
        order_y = jnp.array(ORDER_Y_FIRST, jnp.int32) ^ me
        place_x = jnp.array([ORDER_X_FIRST.index(i) for i in range(8)], jnp.int32)[lanes ^ me]
        place_y = jnp.array([ORDER_Y_FIRST.index(i) for i in range(8)], jnp.int32)[lanes ^ me]
        layers = (shards[:10], shards[10:])

        def in_shard(p):
            rows = p[1].shape[0]
            parts = [p[1].reshape(rows, 8, 256), p[2].reshape(rows, 8, 128), p[3].reshape(rows, 8, 128)]
            qkv = jnp.concatenate(parts, axis=2).reshape(rows, 4096)
            return jnp.concatenate([p[5], p[6]], axis=1), qkv

        def out_shard(p):
            return jnp.concatenate([p[4], p[7]], axis=0)[None]

        one, two = layers
        vectors = gather(jnp.concatenate([one[0], one[8], one[9], two[0], two[8], two[9]])[None])
        in_1 = gather(jnp.concatenate(in_shard(one), axis=1))
        out_1 = gather(out_shard(one))
        gu_2, qkv_2 = in_shard(two)
        gu_2 = gather(gu_2)
        out_2 = gather(out_shard(two))
        qkv_2 = gather(qkv_2)
        w_gu, w_qkv, w_out = (in_1, gu_2), ((in_1, 6144), (qkv_2, 0)), (out_1, out_2)
        gains = []
        for base in (0, 512):
            gains.append((vectors[:, base:base + 128].reshape(-1),
                          vectors[:, base + 128:base + 384].reshape(8, 2, 128),
                          vectors[:, base + 384:base + 512].reshape(8, 1, 128)))

        inv_freq = ROPE_THETA ** (-jnp.arange(0, HEAD_DIM, 2, dtype=F32) / HEAD_DIM)
        angles = positions.astype(F32)[:, None] * jnp.repeat(inv_freq, 2)[None, :]
        cos = jnp.cos(angles)
        sin = jnp.sin(angles) * jnp.where(jnp.arange(HEAD_DIM) % 2 == 0, -1.0, 1.0)[None, :]

        stream = x_in[0]
        saved = []
        for index in range(2):
            ln_gain, q_gain, k_gain = gains[index]
            normed, normed_x, normed_y = norm_blocks(stream, ln_gain, order_x, order_y)
            gate, up, *hidden = swiglu_forward(normed, w_gu[index], 0, 3072, place_x, place_y)
            *heads, attn, attn_placed = attention_forward(normed, *w_qkv[index], q_gain, k_gain, cos, sin,
                                                          place_y if index else place_x)
            saved.append((stream, normed_x, normed_y, heads, attn_placed, gate, up, hidden))
            stream = output_projection(stream, attn, hidden[0], w_out[index])
        y_out = stream

        grad = grad_out[0]
        results = [None, None]
        vector_parts = [None, None]
        for index in (1, 0):
            ln_gain, q_gain, k_gain = gains[index]
            stream, normed_x, normed_y, heads, attn, gate, up, hidden = saved[index]
            if index:
                g_down = jnp.concatenate([reduce_product(hidden[1], grad[:, :512], True),
                                          reduce_product(hidden[2], grad[:, 512:], False)], axis=1)
            else:
                g_down = reduce_product(hidden[2], grad, False)
            d_attn, d_gate, d_up = output_backward(grad, w_out[index], gate, up, attn.shape[1])
            g_gate = reduce_product(normed_x, d_gate, True)
            g_up = reduce_product(normed_y, d_up, False)
            g_o = reduce_product(attn, grad, index == 0)
            d_qkv_a, *g_norms_a = attention_backward(*heads, d_attn, q_gain, k_gain, cos, sin, 0, 4)
            d_qkv_b, *g_norms_b = attention_backward(*heads, d_attn, q_gain, k_gain, cos, sin, 4, 4)
            g_qn, g_kn = (jnp.concatenate(pair) for pair in zip(g_norms_a, g_norms_b))
            g_qkv = jnp.concatenate([reduce_product(normed_x, d_qkv_a, True),
                                     reduce_product(normed_y, d_qkv_b, False)], axis=1)
            grad, g_ln = input_backward(d_gate, d_up, d_qkv_a, d_qkv_b, w_gu[index], *w_qkv[index],
                                        stream, ln_gain, grad)
            vector_parts[index] = [g_ln.reshape(8, 128), g_qn.reshape(8, 256), g_kn.reshape(8, 128)]
            split = g_qkv.reshape(128, 8, 512)
            results[index] = [split[:, :, :256].reshape(128, 2048), split[:, :, 256:384].reshape(128, 1024),
                              split[:, :, 384:].reshape(128, 1024), g_o, g_gate, g_up, g_down]
        g_vec = reduce_vector(jnp.concatenate(vector_parts[0] + vector_parts[1], axis=1))
        outs = []
        for index in range(2):
            part = g_vec[512 * index:512 * (index + 1)]
            outs += [part[:128]] + results[index] + [part[128:384], part[384:]]
        return (y_out[None], grad[None], *outs)

    return jax.shard_map(body, mesh=mesh, in_specs=in_specs, out_specs=out_specs, check_vma=False)
```
